64 devices in a mesh: dp: 4 (over x, y), ctx: 16 (over z, core).
Axes of the slice: x: 2, y: 2, z: 8, core: 2. Of those that a mesh axis runs over, the one named last changes fastest.
The devices are a block of a 4x4x8 slice.
Arguments:
- x_chunk: bfloat16 [32768, 1152], P(('dp', 'ctx')), parts along dimension 0
- cache_len: int32 [4], P('dp'), parts along dimension 0
- k_cache: bfloat16 [2, 32768, 1, 256], P(None, ('dp', 'ctx')), parts along dimension 1
- v_cache: bfloat16 [2, 32768, 1, 256], P(None, ('dp', 'ctx')), parts along dimension 1
- k_local: bfloat16 [2, 2048, 1, 256], P(None, 'dp'), parts along dimension 1
- v_local: bfloat16 [2, 2048, 1, 256], P(None, 'dp'), parts along dimension 1
- g_attn: bfloat16 [4, 1152], replicated
- g_mlp: bfloat16 [4, 1152], replicated
- w_q: bfloat16 [4, 1152, 1024], replicated
- w_k: bfloat16 [4, 1152, 256], replicated
- w_v: bfloat16 [4, 1152, 256], replicated
- w_o: bfloat16 [4, 1024, 1152], replicated
- w_gate: bfloat16 [4, 1152, 6912], replicated
- w_up: bfloat16 [4, 1152, 6912], replicated
- w_down: bfloat16 [4, 6912, 1152], replicated
Outputs:
- output: bfloat16 [32768, 1152], P(('dp', 'ctx')), parts along dimension 0
There are 4 independent parts. The reference program is written for one: setup_inputs(seed, part) draws one part's arguments, and reference() takes and returns one part's arrays. A program takes and returns all parts, laid end to end along the dimension named above; an argument that names none is the same for every part.
All inputs are finite; a program needn't handle non-finite values.
Results may differ from the reference program's by a relative error of at most 0.02.
Values are sent between devices in bfloat16 or wider.
A program may use at most 768 MiB of HBM per device.

```python
import math
import jax
import jax.numpy as jnp
from jax import lax

D_MODEL = 1152
NUM_HEADS = 4
KV_HEADS = 1
HEAD_DIM = 256
WINDOW = 512
FF_DIM = 6912
SEQ_NEW = 8192
CACHE_SIZE = 8192
QUERY_ROWS = 128
NUM_PAIRS = 2
NORM_EPS = 1e-6


def draw_normal(rng_key, arr_shape, factor):
    return jax.random.normal(rng_key, arr_shape, jnp.float32) * factor


def setup_inputs(seed: int = 0, part: int = 0) -> dict:
    part_keys = jax.random.split(jax.random.fold_in(jax.random.key(seed), part), 6)
    shared_keys = jax.random.split(jax.random.key(seed + 1), 9)
    n_layers = 2 * NUM_PAIRS
    q_width = NUM_HEADS * HEAD_DIM
    kv_width = KV_HEADS * HEAD_DIM
    gain_local = math.log(max(WINDOW / 8.0, 2.0)) ** 0.25
    gain_global = math.log(max((CACHE_SIZE + SEQ_NEW) / 16.0, 2.0)) ** 0.25
    gain_base = jnp.tile(jnp.array([gain_local, gain_global], jnp.float32), NUM_PAIRS)
    cache_shape = (NUM_PAIRS, CACHE_SIZE, KV_HEADS, HEAD_DIM)
    local_shape = (NUM_PAIRS, WINDOW, KV_HEADS, HEAD_DIM)
    x_chunk = draw_normal(part_keys[0], (SEQ_NEW, D_MODEL), 1.0).astype(jnp.bfloat16)
    cache_len = jax.random.randint(part_keys[1], (1,), CACHE_SIZE // 2, CACHE_SIZE + 1, jnp.int32)
    k_cache = draw_normal(part_keys[2], cache_shape, gain_global).astype(jnp.bfloat16)
    v_cache = draw_normal(part_keys[3], cache_shape, gain_global).astype(jnp.bfloat16)
    k_local = draw_normal(part_keys[4], local_shape, gain_local).astype(jnp.bfloat16)
    v_local = draw_normal(part_keys[5], local_shape, gain_local).astype(jnp.bfloat16)
    g_attn = (gain_base[:, None] * (1.0 + draw_normal(shared_keys[0], (n_layers, D_MODEL), 0.2))).astype(jnp.bfloat16)
    g_mlp = (1.0 + draw_normal(shared_keys[1], (n_layers, D_MODEL), 0.2)).astype(jnp.bfloat16)
    w_q = draw_normal(shared_keys[2], (n_layers, D_MODEL, q_width), D_MODEL ** -0.5).astype(jnp.bfloat16)
    w_k = draw_normal(shared_keys[3], (n_layers, D_MODEL, kv_width), D_MODEL ** -0.5).astype(jnp.bfloat16)
    w_v = draw_normal(shared_keys[4], (n_layers, D_MODEL, kv_width), D_MODEL ** -0.5).astype(jnp.bfloat16)
    w_o = draw_normal(shared_keys[5], (n_layers, q_width, D_MODEL), q_width ** -0.5).astype(jnp.bfloat16)
    w_gate = draw_normal(shared_keys[6], (n_layers, D_MODEL, FF_DIM), D_MODEL ** -0.5).astype(jnp.bfloat16)
    w_up = draw_normal(shared_keys[7], (n_layers, D_MODEL, FF_DIM), D_MODEL ** -0.5).astype(jnp.bfloat16)
    w_down = draw_normal(shared_keys[8], (n_layers, FF_DIM, D_MODEL), FF_DIM ** -0.5).astype(jnp.bfloat16)
    return {'x_chunk': x_chunk, 'cache_len': cache_len, 'k_cache': k_cache, 'v_cache': v_cache,
            'k_local': k_local, 'v_local': v_local, 'g_attn': g_attn, 'g_mlp': g_mlp,
            'w_q': w_q, 'w_k': w_k, 'w_v': w_v, 'w_o': w_o,
            'w_gate': w_gate, 'w_up': w_up, 'w_down': w_down}


def rms_norm(rows_in, gain_vec):
    rows_f32 = rows_in.astype(jnp.float32)
    inv_rms = lax.rsqrt(jnp.mean(rows_f32 * rows_f32, axis=-1, keepdims=True) + NORM_EPS)
    return (rows_f32 * inv_rms * gain_vec.astype(jnp.float32)).astype(jnp.bfloat16)


def project(rows_in, weight):
    return jnp.dot(rows_in, weight, preferred_element_type=jnp.float32).astype(jnp.bfloat16)


def qkv_heads(normed, w_query, w_key, w_value):
    groups = NUM_HEADS // KV_HEADS
    queries = project(normed, w_query).reshape(SEQ_NEW, KV_HEADS, groups, HEAD_DIM)
    new_k = project(normed, w_key).reshape(SEQ_NEW, KV_HEADS, HEAD_DIM)
    new_v = project(normed, w_value).reshape(SEQ_NEW, KV_HEADS, HEAD_DIM)
    return queries, new_k, new_v


def attend(score_list, value_list):
    row_max = score_list[0].max(axis=-1)
    for part_scores in score_list[1:]:
        row_max = jnp.maximum(row_max, part_scores.max(axis=-1))
    row_sum = 0.0
    weighted = 0.0
    for part_scores, part_values in zip(score_list, value_list):
        part_probs = jnp.exp(part_scores - row_max[..., None])
        row_sum = row_sum + part_probs.sum(axis=-1)
        weighted = weighted + jnp.einsum('hgqk,khd->qhgd', part_probs.astype(jnp.bfloat16).astype(jnp.float32), part_values.astype(jnp.float32))
    return (weighted / jnp.transpose(row_sum, (2, 0, 1))[..., None]).astype(jnp.bfloat16)


def local_attention(queries, ext_k, ext_v):
    score_scale = HEAD_DIM ** -0.5
    rel_pos = jnp.arange(WINDOW + QUERY_ROWS)[None, :] - jnp.arange(QUERY_ROWS)[:, None]
    band_mask = (rel_pos > 0) & (rel_pos <= WINDOW)

    def one_block(block_idx):
        row_start = block_idx * QUERY_ROWS
        q_rows = lax.dynamic_slice_in_dim(queries, row_start, QUERY_ROWS, axis=0).astype(jnp.float32)
        k_rows = lax.dynamic_slice_in_dim(ext_k, row_start, WINDOW + QUERY_ROWS, axis=0)
        v_rows = lax.dynamic_slice_in_dim(ext_v, row_start, WINDOW + QUERY_ROWS, axis=0)
        scores = jnp.einsum('qhgd,khd->hgqk', q_rows, k_rows.astype(jnp.float32)) * score_scale
        scores = jnp.where(band_mask, scores, -jnp.inf)
        return attend([scores], [v_rows])

    blocks = lax.map(one_block, jnp.arange(SEQ_NEW // QUERY_ROWS))
    return blocks.reshape(SEQ_NEW, NUM_HEADS * HEAD_DIM)


def global_attention(queries, cache_k, cache_v, new_k, new_v, valid_len):
    score_scale = HEAD_DIM ** -0.5
    cache_mask = jnp.arange(CACHE_SIZE) < valid_len
    new_pos = jnp.arange(SEQ_NEW)
    cache_f32 = cache_k.astype(jnp.float32)
    new_f32 = new_k.astype(jnp.float32)

    def one_block(block_idx):
        row_start = block_idx * QUERY_ROWS
        q_rows = lax.dynamic_slice_in_dim(queries, row_start, QUERY_ROWS, axis=0).astype(jnp.float32)
        q_pos = row_start + jnp.arange(QUERY_ROWS)
        cache_scores = jnp.einsum('qhgd,khd->hgqk', q_rows, cache_f32) * score_scale
        cache_scores = jnp.where(cache_mask, cache_scores, -jnp.inf)
        new_scores = jnp.einsum('qhgd,khd->hgqk', q_rows, new_f32) * score_scale
        new_scores = jnp.where(new_pos[None, :] <= q_pos[:, None], new_scores, -jnp.inf)
        return attend([cache_scores, new_scores], [cache_v, new_v])

    blocks = lax.map(one_block, jnp.arange(SEQ_NEW // QUERY_ROWS))
    return blocks.reshape(SEQ_NEW, NUM_HEADS * HEAD_DIM)


def add_residual(hidden, attn_out, w_out):
    return (hidden.astype(jnp.float32) + jnp.dot(attn_out, w_out, preferred_element_type=jnp.float32)).astype(jnp.bfloat16)


def mlp_block(hidden, gain_vec, w_gate, w_up, w_down):
    normed = rms_norm(hidden, gain_vec)
    gate_pre = jnp.dot(normed, w_gate, preferred_element_type=jnp.float32)
    up_pre = jnp.dot(normed, w_up, preferred_element_type=jnp.float32)
    act_bf16 = (jax.nn.gelu(gate_pre, approximate=True) * up_pre).astype(jnp.bfloat16)
    return (hidden.astype(jnp.float32) + jnp.dot(act_bf16, w_down, preferred_element_type=jnp.float32)).astype(jnp.bfloat16)


def reference(x_chunk, cache_len, k_cache, v_cache, k_local, v_local, g_attn, g_mlp, w_q, w_k, w_v, w_o, w_gate, w_up, w_down):
    hidden = x_chunk
    for pair_idx in range(NUM_PAIRS):
        layer_idx = 2 * pair_idx
        queries, new_k, new_v = qkv_heads(rms_norm(hidden, g_attn[layer_idx]), w_q[layer_idx], w_k[layer_idx], w_v[layer_idx])
        ext_k = jnp.concatenate([k_local[pair_idx], new_k], axis=0)
        ext_v = jnp.concatenate([v_local[pair_idx], new_v], axis=0)
        attn_out = local_attention(queries, ext_k, ext_v)
        hidden = add_residual(hidden, attn_out, w_o[layer_idx])
        hidden = mlp_block(hidden, g_mlp[layer_idx], w_gate[layer_idx], w_up[layer_idx], w_down[layer_idx])
        layer_idx = 2 * pair_idx + 1
        queries, new_k, new_v = qkv_heads(rms_norm(hidden, g_attn[layer_idx]), w_q[layer_idx], w_k[layer_idx], w_v[layer_idx])
        attn_out = global_attention(queries, k_cache[pair_idx], v_cache[pair_idx], new_k, new_v, cache_len[0])
        hidden = add_residual(hidden, attn_out, w_o[layer_idx])
        hidden = mlp_block(hidden, g_mlp[layer_idx], w_gate[layer_idx], w_up[layer_idx], w_down[layer_idx])
    return hidden
```

```python
import functools
import jax
import jax.numpy as jnp
from jax import lax
from jax.sharding import PartitionSpec as P
from jax.experimental import pallas as pl
from jax.experimental.pallas import tpu as pltpu

NORM_EPS = 1e-6
LOG2E = 1.4426950408889634
NEG = -1e30
BF = 768
NS = 3


def rms_rows(x, gain):
    xf = x.astype(jnp.float32)
    inv = lax.rsqrt(jnp.mean(xf * xf, axis=-1, keepdims=True) + NORM_EPS)
    return (xf * inv * gain.astype(jnp.float32)).astype(jnp.bfloat16)


def dotf(a, b):
    return jnp.dot(a, b, preferred_element_type=jnp.float32)


def dot_t(a, b):
    return lax.dot_general(a, b, (((1,), (1,)), ((), ())), preferred_element_type=jnp.float32)


def dense_call(stages, x, weights, q=None, k=None, v=None, halo_k=None, halo_v=None, attn=None, heads=4, name="dense"):
    g_attn, g_mlp, w_q, w_k, w_v, w_o, w_gate, w_up, w_down = weights
    rows, width = x.shape
    ff = w_gate.shape[-1]
    qw = w_q.shape[-1]
    kw = w_k.shape[-1]
    nb = ff // BF
    names = [s for s, _ in stages]
    has_l = "lattn" in names
    mlps = [l for s, l in stages if s == "mlp"]
    qkvs = [l for s, l in stages if s == "qkv"]
    oprojs = [l for s, l in stages if s == "oproj"]
    scale = kw ** -0.5 * LOG2E

    ins = [x, g_attn, g_mlp]
    vm = pl.BlockSpec(memory_space=pltpu.VMEM)
    hb = pl.BlockSpec(memory_space=pl.ANY)
    specs = [vm] * 3
    if has_l:
        ins += [q, k, v, halo_k, halo_v]
        specs += [vm] * 5
    elif attn is not None:
        ins += [attn]
        specs += [vm]
    n_small = len(ins)
    ins += [w_q, w_k, w_v, w_o, w_gate, w_up, w_down]
    specs += [hb] * 7
    outs = [jax.ShapeDtypeStruct((rows, width), jnp.bfloat16)]
    if qkvs:
        outs += [jax.ShapeDtypeStruct((rows, qw), jnp.bfloat16), jax.ShapeDtypeStruct((rows, kw), jnp.bfloat16), jax.ShapeDtypeStruct((rows, kw), jnp.bfloat16)]
    scratch = dict(
        xs=pltpu.VMEM((rows, width), jnp.bfloat16),
        hs=pltpu.VMEM((rows, width), jnp.bfloat16),
        acc=pltpu.VMEM((rows, width), jnp.float32),
        os=pltpu.VMEM((rows, qw), jnp.bfloat16),
        wqb=pltpu.VMEM((width, qw), jnp.bfloat16),
        wkb=pltpu.VMEM((width, kw), jnp.bfloat16),
        wvb=pltpu.VMEM((width, kw), jnp.bfloat16),
        wob=pltpu.VMEM((qw, width), jnp.bfloat16),
        wgb=pltpu.VMEM((NS, width, BF), jnp.bfloat16),
        wub=pltpu.VMEM((NS, width, BF), jnp.bfloat16),
        wdb=pltpu.VMEM((NS, BF, width), jnp.bfloat16),
        msem=pltpu.SemaphoreType.DMA((3, NS)),
        psem=pltpu.SemaphoreType.DMA((4,)),
    )
    if has_l:
        scratch.update(kx=pltpu.VMEM((2 * rows, kw), jnp.bfloat16), vx=pltpu.VMEM((2 * rows, kw), jnp.bfloat16))
    keys = list(scratch)

    def kernel(*refs):
        x_ref, ga_ref, gm_ref = refs[:3]
        if has_l:
            q_ref, k_ref, v_ref, hk_ref, hv_ref = refs[3:8]
        elif attn is not None:
            a_ref = refs[3]
        wq_h, wk_h, wv_h, wo_h, wg_h, wu_h, wd_h = refs[n_small:n_small + 7]
        o_refs = refs[n_small + 7:n_small + 7 + len(outs)]
        sc = dict(zip(keys, refs[n_small + 7 + len(outs):]))
        xs, hs, acc, os_ = sc["xs"], sc["hs"], sc["acc"], sc["os"]

        def wcopies(l, j, slot):
            off = pl.multiple_of(j * BF, BF)
            return [
                pltpu.make_async_copy(wg_h.at[l, :, pl.ds(off, BF)], sc["wgb"].at[slot], sc["msem"].at[0, slot]),
                pltpu.make_async_copy(wu_h.at[l, :, pl.ds(off, BF)], sc["wub"].at[slot], sc["msem"].at[1, slot]),
                pltpu.make_async_copy(wd_h.at[l, pl.ds(off, BF), :], sc["wdb"].at[slot], sc["msem"].at[2, slot]),
            ]

        def start_mlp(l):
            for j in range(NS - 1):
                for c in wcopies(l, j, j):
                    c.start()

        def qkv_copies(l):
            return [pltpu.make_async_copy(src.at[l], sc[dst], sc["psem"].at[i]) for i, (src, dst) in enumerate([(wq_h, "wqb"), (wk_h, "wkb"), (wv_h, "wvb")])]

        def o_copy(l):
            return pltpu.make_async_copy(wo_h.at[l], sc["wob"], sc["psem"].at[3])

        if oprojs:
            o_copy(oprojs[0]).start()
        if stages[0][0] == "qkv":
            for c in qkv_copies(qkvs[0]):
                c.start()
        if mlps:
            start_mlp(mlps[0])
        if qkvs and stages[0][0] != "qkv":
            for c in qkv_copies(qkvs[0]):
                c.start()
        if "oproj" not in names and "mlp" not in names:
            xs_src = x_ref
        else:
            xs_src = None
        cur = [x_ref]

        def do_lattn(l):
            half = rows // 2
            sc["kx"][0:rows, :] = hk_ref[...]
            sc["kx"][rows:2 * rows, :] = k_ref[...]
            sc["vx"][0:rows, :] = hv_ref[...]
            sc["vx"][rows:2 * rows, :] = v_ref[...]
            span = rows + half
            ri = lax.broadcasted_iota(jnp.int32, (half, span), 0)
            ci = lax.broadcasted_iota(jnp.int32, (half, span), 1)
            ok = (ci > ri) & (ci <= ri + rows)
            for t in range(2):
                for h in range(heads):
                    qt = q_ref[t * half:(t + 1) * half, h * kw:(h + 1) * kw]
                    s = dot_t(qt, sc["kx"][t * half:t * half + span, :])
                    s = jnp.where(ok, s, NEG)
                    m = jnp.max(s, axis=1, keepdims=True)
                    p = jnp.exp2((s - m) * scale)
                    den = jnp.sum(p, axis=1, keepdims=True)
                    num = dotf(p.astype(jnp.bfloat16), sc["vx"][t * half:t * half + span, :])
                    os_[t * half:(t + 1) * half, h * kw:(h + 1) * kw] = (num / den).astype(jnp.bfloat16)

        def do_oproj(l):
            src = os_ if has_l else a_ref
            o_copy(l).wait()
            xs[...] = (cur[0][...].astype(jnp.float32) + dotf(src[...], sc["wob"][...])).astype(jnp.bfloat16)
            cur[0] = xs

        def do_mlp(l):
            hs[...] = rms_rows(cur[0][...], gm_ref[l:l + 1, :])
            acc[...] = cur[0][...].astype(jnp.float32)

            def step(j, slot, nxt_slot):
                for c in wcopies(l, j, slot):
                    c.wait()

                @pl.when(j + NS - 1 < nb)
                def _():
                    for c in wcopies(l, j + NS - 1, nxt_slot):
                        c.start()
                ga = dotf(hs[...], sc["wgb"][slot])
                up = dotf(hs[...], sc["wub"][slot])
                a = (jax.nn.gelu(ga, approximate=True) * up).astype(jnp.bfloat16)
                acc[...] += dotf(a, sc["wdb"][slot])

            def loop(jj, _):
                for s in range(NS):
                    step(jj * NS + s, s, (s + NS - 1) % NS)
                return 0
            lax.fori_loop(0, nb // NS, loop, 0)
            xs[...] = acc[...].astype(jnp.bfloat16)
            cur[0] = xs

        def do_qkv(l):
            hs[...] = rms_rows(cur[0][...], ga_ref[l:l + 1, :])
            for c in qkv_copies(l):
                c.wait()
            o_refs[2][...] = dotf(hs[...], sc["wkb"][...]).astype(jnp.bfloat16)
            o_refs[3][...] = dotf(hs[...], sc["wvb"][...]).astype(jnp.bfloat16)
            o_refs[1][...] = dotf(hs[...], sc["wqb"][...]).astype(jnp.bfloat16)

        for s, l in stages:
            dict(lattn=do_lattn, oproj=do_oproj, mlp=do_mlp, qkv=do_qkv)[s](l)
        o_refs[0][...] = cur[0][...]

    flops = 0
    for s, l in stages:
        flops += 2 * rows * width * {"mlp": 3 * ff, "qkv": qw + 2 * kw, "oproj": qw, "lattn": 4 * rows}[s]
    return pl.pallas_call(
        kernel, out_shape=tuple(outs), in_specs=specs, out_specs=tuple([vm] * len(outs)),
        scratch_shapes=list(scratch.values()),
        cost_estimate=pl.CostEstimate(flops=flops, bytes_accessed=len(mlps) * 3 * width * ff * 2 + 10**6, transcendentals=0),
        compiler_params=pltpu.CompilerParams(vmem_limit_bytes=60 * 1024 * 1024), name=name)(*ins)


MESH = pl.DeviceIdType.MESH
CB = 1024


def flash_units(q_ref, m_ref, l_ref, acc_ref, s_scr, k_of, v_of, keys, mask, heads, dim, scale):
    def scores(h):
        return dot_t(q_ref[:, h * dim:(h + 1) * dim], k_of())
    s_scr[0, :, 0:keys] = scores(0)
    for h in range(heads):
        if h + 1 < heads:
            s_scr[(h + 1) % 2, :, 0:keys] = scores(h + 1)
        s = s_scr[h % 2, :, 0:keys]
        if mask is not None:
            s = jnp.where(mask, s, -jnp.inf)
        m_prev = m_ref[h]
        mx = s[:, 0:128]
        for c in range(1, keys // 128):
            mx = jnp.maximum(mx, s[:, c * 128:(c + 1) * 128])
        m_cur = jnp.maximum(m_prev, jnp.max(mx, axis=1, keepdims=True))
        alpha = jnp.exp2((m_prev - m_cur) * scale)
        lsum = alpha * l_ref[h]
        parts = []
        for c in range(keys // 128):
            e = jnp.exp2((s[:, c * 128:(c + 1) * 128] - m_cur) * scale)
            lsum = lsum + e
            parts.append(e.astype(jnp.bfloat16))
        l_ref[h] = lsum
        m_ref[h] = m_cur
        pv = dotf(jnp.concatenate(parts, axis=1), v_of())
        for c in range(dim // 128):
            lo = h * dim + c * 128
            acc_ref[:, lo:lo + 128] = acc_ref[:, lo:lo + 128] * alpha + pv[:, c * 128:(c + 1) * 128]


def global_call(q, k, v, ck, cv, clen, n_ctx, heads=4):
    rows, qw = q.shape
    dim = k.shape[1]
    slots = ck.shape[0]
    ncb = slots // CB
    n_chip = n_ctx // 2
    scale = dim ** -0.5 * LOG2E
    n_arr = 2 * (n_chip - 1)

    def kernel(clen_ref, q_ref, k_ref, v_ref, ck_h, cv_h, o_ref, kv, m_ref, l_ref, acc_ref, s_scr, cb, csem, rs, rr, ps, pr):
        me = lax.axis_index("ctx")
        z, p = me // 2, me % 2
        step_dir = 1 - 2 * p
        partner = z * 2 + (1 - p)
        succ = ((z + step_dir + n_chip) % n_chip) * 2 + p
        pred = ((z - step_dir + n_chip) % n_chip) * 2 + p

        def mine(s):
            return ((z - step_dir * s + n_chip) % n_chip) * 2 + p

        def theirs(s):
            return ((z + step_dir * s + n_chip) % n_chip) * 2 + (1 - p)

        barrier = pltpu.get_barrier_semaphore()
        for who in (pred, partner):
            pl.semaphore_signal(barrier, inc=1, device_id={"ctx": who}, device_id_type=MESH)
        pl.semaphore_wait(barrier, 2)

        own = (k_ref, v_ref)

        def own_send(t, who, ss, rsem, i):
            return pltpu.make_async_remote_copy(src_ref=own[t], dst_ref=kv.at[t, me], send_sem=ss.at[i], recv_sem=rsem.at[i], device_id={"ctx": who}, device_id_type=MESH)

        def fwd(a, who, ss, rsem, i):
            d = mine(a // 2 + 1)
            return pltpu.make_async_remote_copy(src_ref=kv.at[a % 2, d], dst_ref=kv.at[a % 2, d], send_sem=ss.at[i], recv_sem=rsem.at[i], device_id={"ctx": who}, device_id_type=MESH)

        for t in range(2):
            own_send(t, succ, rs, rr, t).start()
        for t in range(2):
            own_send(t, partner, ps, pr, t).start()

        def wait_arrival(a):
            d = mine(a // 2 + 1)
            pltpu.make_async_remote_copy(src_ref=kv.at[a % 2, d], dst_ref=kv.at[a % 2, d], send_sem=rs.at[a], recv_sem=rr.at[a], device_id={"ctx": pred}, device_id_type=MESH).wait_recv()

        def wait_partner(t, s):
            d = theirs(s)
            pltpu.make_async_remote_copy(src_ref=kv.at[t, d], dst_ref=kv.at[t, d], send_sem=ps.at[2 * s + t], recv_sem=pr.at[2 * s + t], device_id={"ctx": partner}, device_id_type=MESH).wait_recv()

        def handle(a):
            wait_arrival(a)

            @pl.when(a + 2 < n_arr)
            def _():
                fwd(a, succ, rs, rr, a + 2).start()
            fwd(a, partner, ps, pr, a + 2).start()

        def ccopy(i):
            off = pl.multiple_of(i * CB, CB)
            return [pltpu.make_async_copy(src.at[pl.ds(off, CB), :], cb.at[t, i % 2], csem.at[t, i % 2]) for t, src in ((0, ck_h), (1, cv_h))]

        for c in ccopy(0):
            c.start()
        m_ref[...] = jnp.full_like(m_ref, -jnp.inf)
        l_ref[...] = jnp.zeros_like(l_ref)
        acc_ref[...] = jnp.zeros_like(acc_ref)
        units = functools.partial(flash_units, q_ref, m_ref, l_ref, acc_ref, s_scr, heads=heads, dim=dim, scale=scale)
        ri = lax.broadcasted_iota(jnp.int32, (rows, rows), 0)
        ci = lax.broadcasted_iota(jnp.int32, (rows, rows), 1)
        units(lambda: k_ref[...], lambda: v_ref[...], rows, ci <= ri)

        def cache_step(masked):
            def body(i, carry):
                for c in ccopy(i):
                    c.wait()

                @pl.when(i + 1 < ncb)
                def _():
                    for c in ccopy(i + 1):
                        c.start()

                @pl.when(i >= 1)
                def _():
                    handle(i - 1)
                mask = None
                if masked:
                    mask = (lax.broadcasted_iota(jnp.int32, (1, CB), 1) + i * CB) < clen_ref[0]
                units(lambda: cb[0, i % 2], lambda: cb[1, i % 2], CB, mask)
                return carry
            return body
        lax.fori_loop(0, ncb // 2, cache_step(False), 0)
        lax.fori_loop(ncb // 2, ncb, cache_step(True), 0)

        def shard(d):
            @pl.when(d < me)
            def _():
                units(lambda: kv[0, d], lambda: kv[1, d], rows, None)

        wait_partner(0, 0)
        wait_partner(1, 0)
        shard(partner)

        def new_step(s, carry):
            @pl.when(s + ncb - 2 < n_arr)
            def _():
                handle(s + ncb - 2)
            shard(mine(s))
            wait_partner(0, s)
            wait_partner(1, s)
            shard(theirs(s))
            return carry
        lax.fori_loop(1, n_chip, new_step, 0)

        for t in range(2):
            own_send(t, succ, rs, rr, t).wait_send()
            own_send(t, partner, ps, pr, t).wait_send()

        def drain(a, carry):
            @pl.when(a + 2 < n_arr)
            def _():
                fwd(a, succ, rs, rr, a + 2).wait_send()
            fwd(a, partner, ps, pr, a + 2).wait_send()
            return carry
        lax.fori_loop(0, n_arr, drain, 0)
        for h in range(heads):
            den = jnp.sum(l_ref[h], axis=1, keepdims=True)
            o_ref[:, h * dim:(h + 1) * dim] = (acc_ref[:, h * dim:(h + 1) * dim] / den).astype(jnp.bfloat16)

    vm = pl.BlockSpec(memory_space=pltpu.VMEM)
    hb = pl.BlockSpec(memory_space=pl.ANY)
    sem = pltpu.SemaphoreType.DMA
    return pl.pallas_call(
        kernel, out_shape=jax.ShapeDtypeStruct((rows, qw), jnp.bfloat16),
        in_specs=[pl.BlockSpec(memory_space=pltpu.SMEM), vm, vm, vm, hb, hb], out_specs=vm,
        scratch_shapes=[
            pltpu.VMEM((2, n_ctx, rows, dim), jnp.bfloat16),
            pltpu.VMEM((heads, rows, 128), jnp.float32), pltpu.VMEM((heads, rows, 128), jnp.float32),
            pltpu.VMEM((rows, qw), jnp.float32), pltpu.VMEM((2, rows, CB), jnp.float32),
            pltpu.VMEM((2, 2, CB, dim), jnp.bfloat16), sem((2, 2)),
            sem((n_arr,)), sem((n_arr,)), sem((n_arr + 2,)), sem((n_arr + 2,))],
        cost_estimate=pl.CostEstimate(flops=4 * rows * qw * (slots + n_ctx * rows), bytes_accessed=4 * slots * dim, transcendentals=0),
        compiler_params=pltpu.CompilerParams(vmem_limit_bytes=60 * 1024 * 1024, collective_id=1, has_side_effects=True), name="gattn")(clen, q, k, v, ck, cv)


def solution(mesh):
    n_ctx = mesh.shape['ctx']
    shift_pairs = [(i, i + 1) for i in range(n_ctx - 1)]
    row_spec = P(('dp', 'ctx'), None)
    cache_spec = P(None, ('dp', 'ctx'), None, None)
    local_spec = P(None, 'dp', None, None)
    in_specs = (row_spec, P('dp'), cache_spec, cache_spec, local_spec, local_spec) + (P(),) * 9

    def device_step(x, cache_len, k_cache, v_cache, k_local, v_local, g_attn, g_mlp, w_q, w_k, w_v, w_o, w_gate, w_up, w_down):
        weights = (g_attn, g_mlp, w_q, w_k, w_v, w_o, w_gate, w_up, w_down)
        is_first = lax.axis_index('ctx') == 0
        n_pairs = k_cache.shape[0]
        caches = [[lax.all_gather(c[i, :, 0, :], 'ctx', axis=0, tiled=True) for c in (k_cache, v_cache)] for i in range(n_pairs)]
        _, q, k, v = dense_call([("qkv", 0)], x, weights, name="qkv")
        for i in range(n_pairs):
            halo_k = jnp.where(is_first, k_local[i, :, 0, :], lax.ppermute(k, 'ctx', shift_pairs))
            halo_v = jnp.where(is_first, v_local[i, :, 0, :], lax.ppermute(v, 'ctx', shift_pairs))
            l = 2 * i
            x, q, k, v = dense_call([("lattn", l), ("oproj", l), ("mlp", l), ("qkv", l + 1)], x, weights, q=q, k=k, v=v, halo_k=halo_k, halo_v=halo_v, name="local%d" % i)
            o = global_call(q, k, v, caches[i][0], caches[i][1], cache_len, n_ctx)
            last = i == n_pairs - 1
            r = dense_call([("oproj", l + 1), ("mlp", l + 1)] + ([] if last else [("qkv", l + 2)]), x, weights, attn=o, name="glob%d" % i)
            x = r[0]
            if not last:
                q, k, v = r[1:]
        return x

    return jax.shard_map(device_step, mesh=mesh, in_specs=in_specs, out_specs=row_spec, check_vma=False)
```

```python
import functools
import jax
import jax.numpy as jnp
from jax import lax
from jax.sharding import PartitionSpec as P
from jax.experimental import pallas as pl
from jax.experimental.pallas import tpu as pltpu

NORM_EPS = 1e-6
LOG2E = 1.4426950408889634
MESH = pl.DeviceIdType.MESH
BF = 768
NS = 2


def rms_rows(x, gain):
    xf = x.astype(jnp.float32)
    inv = lax.rsqrt(jnp.mean(xf * xf, axis=-1, keepdims=True) + NORM_EPS)
    return (xf * inv * gain.astype(jnp.float32)).astype(jnp.bfloat16)


def dotf(a, b):
    return jnp.dot(a, b, preferred_element_type=jnp.float32)


def dot_t(a, b):
    return lax.dot_general(a, b, (((1,), (1,)), ((), ())), preferred_element_type=jnp.float32)


def dense_call(stages, x, weights, local=None, caches=None, pair=0, attn=None, heads=4, n_ctx=0, cid=None, name="dense"):
    g_attn, g_mlp, w_q, w_k, w_v, w_o, w_gate, w_up, w_down = weights
    rows, width = x.shape
    ff = w_gate.shape[-1]
    qw = w_q.shape[-1]
    kw = w_k.shape[-1]
    nb = ff // BF
    names = [s for s, _ in stages]
    has_l = "lattn" in names
    mlps = [l for s, l in stages if s == "mlp"]
    qkvs = [l for s, l in stages if s == "qkv"]
    last_qkv = stages[-1][0] == "qkv"
    n_chip = n_ctx // 2
    n_arr = 2 * (n_chip - 1)
    oprojs = [l for s, l in stages if s == "oproj"]
    scale = kw ** -0.5 * LOG2E

    ins = [x, g_attn, g_mlp]
    vm = pl.BlockSpec(memory_space=pltpu.VMEM)
    hb = pl.BlockSpec(memory_space=pl.ANY)
    specs = [vm] * 3
    if attn is not None:
        ins += [attn]
        specs += [vm]
    n_small = len(ins)
    ins += [w_q, w_k, w_v, w_o, w_gate, w_up, w_down]
    specs += [hb] * 7
    if has_l:
        ins += list(local) + list(caches)
        specs += [hb] * 4
    n_in = len(ins)
    outs = [jax.ShapeDtypeStruct((rows, width), jnp.bfloat16)]
    out_specs = [vm]
    if last_qkv:
        out_specs += [vm] * 3
        outs += [jax.ShapeDtypeStruct((rows, qw), jnp.bfloat16), jax.ShapeDtypeStruct((rows, kw), jnp.bfloat16), jax.ShapeDtypeStruct((rows, kw), jnp.bfloat16)]
    scratch = dict(
        xs=pltpu.VMEM((rows, width), jnp.bfloat16),
        hs=pltpu.VMEM((rows, width), jnp.bfloat16),
        acc=pltpu.VMEM((rows, width), jnp.float32),
        os=pltpu.VMEM((rows, qw), jnp.bfloat16),
        wqb=pltpu.VMEM((width, qw), jnp.bfloat16),
        wkb=pltpu.VMEM((width, kw), jnp.bfloat16),
        wvb=pltpu.VMEM((width, kw), jnp.bfloat16),
        wob=pltpu.VMEM((qw, width), jnp.bfloat16),
        wgb=pltpu.VMEM((NS, width, BF), jnp.bfloat16),
        wub=pltpu.VMEM((NS, width, BF), jnp.bfloat16),
        wdb=pltpu.VMEM((NS, BF, width), jnp.bfloat16),
        msem=pltpu.SemaphoreType.DMA((3, NS)),
        psem=pltpu.SemaphoreType.DMA((4,)),
    )
    if has_l:
        outs += [jax.ShapeDtypeStruct((2, n_ctx * rows, kw), jnp.bfloat16)]
        out_specs += [hb]
        scratch.update(
            kvx=pltpu.VMEM((2, 2 * rows, kw), jnp.bfloat16),
            qs=pltpu.VMEM((rows, qw), jnp.bfloat16),
            own=pltpu.VMEM((2, rows, kw), jnp.bfloat16),
            hsem=pltpu.SemaphoreType.DMA((2, 2)),
            osem=pltpu.SemaphoreType.DMA((2, 2)),
            rs=pltpu.SemaphoreType.DMA((n_arr,)), rr=pltpu.SemaphoreType.DMA((n_arr,)),
            ps=pltpu.SemaphoreType.DMA((n_arr + 2,)), pr=pltpu.SemaphoreType.DMA((n_arr + 2,)),
        )
    keys = list(scratch)

    def kernel(*refs):
        x_ref, ga_ref, gm_ref = refs[:3]
        if attn is not None:
            a_ref = refs[3]
        wq_h, wk_h, wv_h, wo_h, wg_h, wu_h, wd_h = refs[n_small:n_small + 7]
        o_refs = refs[n_in:n_in + len(outs)]
        sc = dict(zip(keys, refs[n_in + len(outs):]))
        xs, hs, acc, os_ = sc["xs"], sc["hs"], sc["acc"], sc["os"]
        sent = [0]

        def wcopies(l, j, slot):
            off = pl.multiple_of(j * BF, BF)
            return [
                pltpu.make_async_copy(wg_h.at[l, :, pl.ds(off, BF)], sc["wgb"].at[slot], sc["msem"].at[0, slot]),
                pltpu.make_async_copy(wu_h.at[l, :, pl.ds(off, BF)], sc["wub"].at[slot], sc["msem"].at[1, slot]),
                pltpu.make_async_copy(wd_h.at[l, pl.ds(off, BF), :], sc["wdb"].at[slot], sc["msem"].at[2, slot]),
            ]

        def start_mlp(l):
            for j in range(NS - 1):
                for c in wcopies(l, j, j):
                    c.start()

        def qkv_copies(l):
            return [pltpu.make_async_copy(src.at[l], sc[dst], sc["psem"].at[i]) for i, (src, dst) in enumerate([(wq_h, "wqb"), (wk_h, "wkb"), (wv_h, "wvb")])]

        def o_copy(l):
            return pltpu.make_async_copy(wo_h.at[l], sc["wob"], sc["psem"].at[3])

        if attn is not None:
            o_copy(oprojs[0]).start()
        if qkvs:
            for c in qkv_copies(qkvs[0]):
                c.start()
        if attn is None:
            o_copy(oprojs[0]).start()
        start_mlp(mlps[0])
        cur = [x_ref]

        if has_l:
            kl_h, vl_h, kc_h, vc_h = refs[n_small + 7:n_in]
            cc = o_refs[-1]
            kvx, qs, own = sc["kvx"], sc["qs"], sc["own"]
            hsem, osem, rs, rr, ps, pr = (sc[n] for n in ("hsem", "osem", "rs", "rr", "ps", "pr"))
            me = lax.axis_index("ctx")
            z, p = me // 2, me % 2
            way = 1 - 2 * p
            partner = z * 2 + (1 - p)
            succ = ((z + way + n_chip) % n_chip) * 2 + p
            pred = ((z - way + n_chip) % n_chip) * 2 + p

            def block(t, d):
                return cc.at[t, pl.ds(pl.multiple_of(d * rows, rows), rows), :]

            def mine(a):
                return ((z - way * (a // 2 + 1) + n_chip) % n_chip) * 2 + p

            def theirs(a):
                return ((z + way * (a // 2) + n_chip) % n_chip) * 2 + (1 - p)

            def remote(src, dst, ssem, rsem, who):
                return pltpu.make_async_remote_copy(src_ref=src, dst_ref=dst, send_sem=ssem, recv_sem=rsem, device_id={"ctx": who}, device_id_type=MESH)

            own_in = [pltpu.make_async_copy(src.at[pair], own.at[t], osem.at[0, t]) for t, src in ((0, kc_h), (1, vc_h))]
            own_out = [pltpu.make_async_copy(own.at[t], block(t, me), osem.at[1, t]) for t in range(2)]
            own_ring = [remote(own.at[t], block(t, me), rs.at[t], rr.at[t], succ) for t in range(2)]
            own_part = [remote(own.at[t], block(t, me), ps.at[t], pr.at[t], partner) for t in range(2)]

            def fwd_ring(a):
                return remote(block(a % 2, mine(a)), block(a % 2, mine(a)), rs.at[a + 2], rr.at[a + 2], succ)

            def fwd_part(a):
                return remote(block(a % 2, mine(a)), block(a % 2, mine(a)), ps.at[a + 2], pr.at[a + 2], partner)

            def handle(a):
                remote(block(a % 2, mine(a)), block(a % 2, mine(a)), rs.at[a], rr.at[a], pred).wait_recv()

                @pl.when(a + 2 < n_arr)
                def _():
                    fwd_ring(a).start()
                fwd_part(a).start()

            halo = [remote(kvx.at[t, pl.ds(rows, rows), :], kvx.at[t, pl.ds(0, rows), :], hsem.at[0, t], hsem.at[1, t], me + 1) for t in range(2)]
            halo_in = [remote(kvx.at[t, pl.ds(rows, rows), :], kvx.at[t, pl.ds(0, rows), :], hsem.at[0, t], hsem.at[1, t], me - 1) for t in range(2)]
            first_in = [pltpu.make_async_copy(src.at[pair], kvx.at[t, pl.ds(0, rows), :], hsem.at[1, t]) for t, src in ((0, kl_h), (1, vl_h))]

            for c in own_in:
                c.start()
            barrier = pltpu.get_barrier_semaphore()
            for who in (pred, partner):
                pl.semaphore_signal(barrier, inc=1, device_id={"ctx": who}, device_id_type=MESH)

            @pl.when(p == 0)
            def _():
                pl.semaphore_signal(barrier, inc=1, device_id={"ctx": (me - 1 + n_ctx) % n_ctx}, device_id_type=MESH)

            @pl.when(me == 0)
            def _():
                for c in first_in:
                    c.start()
            pl.semaphore_wait(barrier, 2 + p)
            for t in range(2):
                own_in[t].wait()
                own_ring[t].start()
                own_part[t].start()
                own_out[t].start()

        def do_lattn(l):
            half = rows // 2

            @pl.when(me == 0)
            def _():
                for c in first_in:
                    c.wait()

            @pl.when(me > 0)
            def _():
                for c in halo_in:
                    c.wait_recv()
            span = rows + half
            ri = lax.broadcasted_iota(jnp.int32, (half, span), 0)
            ci = lax.broadcasted_iota(jnp.int32, (half, span), 1)
            ok = (ci > ri) & (ci <= ri + rows)
            for t in range(2):
                for h in range(heads):
                    qt = qs[t * half:(t + 1) * half, h * kw:(h + 1) * kw]
                    s = dot_t(qt, kvx[0, t * half:t * half + span, :])
                    s = jnp.where(ok, s, -jnp.inf)
                    m = jnp.max(s, axis=1, keepdims=True)
                    e = jnp.exp2((s - m) * scale)
                    den = jnp.sum(e, axis=1, keepdims=True)
                    num = dotf(e.astype(jnp.bfloat16), kvx[1, t * half:t * half + span, :])
                    os_[t * half:(t + 1) * half, h * kw:(h + 1) * kw] = (num / den).astype(jnp.bfloat16)

        def do_oproj(l):
            src = a_ref if attn is not None and l == oprojs[0] else os_
            o_copy(l).wait()
            xs[...] = (cur[0][...].astype(jnp.float32) + dotf(src[...], sc["wob"][...])).astype(jnp.bfloat16)
            cur[0] = xs
            if l != oprojs[-1]:
                o_copy(oprojs[-1]).start()

        def do_mlp(l):
            hs[...] = rms_rows(cur[0][...], gm_ref[l:l + 1, :])
            acc[...] = cur[0][...].astype(jnp.float32)

            def step(j, slot, nxt_slot):
                for c in wcopies(l, j, slot):
                    c.wait()

                @pl.when(j + NS - 1 < nb)
                def _():
                    for c in wcopies(l, j + NS - 1, nxt_slot):
                        c.start()
                ga = dotf(hs[...], sc["wgb"][slot])
                up = dotf(hs[...], sc["wub"][slot])
                a = (jax.nn.gelu(ga, approximate=True) * up).astype(jnp.bfloat16)
                acc[...] += dotf(a, sc["wdb"][slot])

            base = sent[0]

            def loop(j, _):
                step(j, lax.rem(j, NS), lax.rem(j + NS - 1, NS))
                if has_l:
                    @pl.when(j + base < n_arr)
                    def _():
                        handle(j + base)
                return 0
            lax.fori_loop(0, nb, loop, 0)
            sent[0] = min(base + nb, n_arr)
            if has_l and l == mlps[-1]:
                for a in range(sent[0], n_arr):
                    handle(a)
                sent[0] = n_arr
            if l != mlps[-1]:
                start_mlp(mlps[-1])
            xs[...] = acc[...].astype(jnp.bfloat16)
            cur[0] = xs

        def do_qkv(l):
            hs[...] = rms_rows(cur[0][...], ga_ref[l:l + 1, :])
            for c in qkv_copies(l):
                c.wait()
            to_local = has_l and l == qkvs[0]
            if to_local:
                kvx[0, rows:2 * rows, :] = dotf(hs[...], sc["wkb"][...]).astype(jnp.bfloat16)
                kvx[1, rows:2 * rows, :] = dotf(hs[...], sc["wvb"][...]).astype(jnp.bfloat16)

                @pl.when(me < n_ctx - 1)
                def _():
                    halo[0].start()
                half_q = qw // 2
                qs[:, 0:half_q] = dotf(hs[...], sc["wqb"][:, 0:half_q]).astype(jnp.bfloat16)

                @pl.when(me < n_ctx - 1)
                def _():
                    halo[1].start()
                qs[:, half_q:qw] = dotf(hs[...], sc["wqb"][:, half_q:qw]).astype(jnp.bfloat16)
                for c in qkv_copies(qkvs[1]):
                    c.start()
            else:
                o_refs[2][...] = dotf(hs[...], sc["wkb"][...]).astype(jnp.bfloat16)
                o_refs[3][...] = dotf(hs[...], sc["wvb"][...]).astype(jnp.bfloat16)
                o_refs[1][...] = dotf(hs[...], sc["wqb"][...]).astype(jnp.bfloat16)

        early = 4 if attn is None else 0
        for s, l in stages:
            dict(lattn=do_lattn, oproj=do_oproj, mlp=do_mlp, qkv=do_qkv)[s](l)
            if early and s == "qkv" and sent[0] == 0:
                handle(0)
                sent[0] = 1
            if early and s == "oproj":
                for a in range(sent[0], early):
                    handle(a)
                sent[0] = early
        o_refs[0][...] = cur[0][...]
        if has_l:
            for t in range(2):
                own_ring[t].wait_send()
                own_part[t].wait_send()
                own_out[t].wait()

            @pl.when(me < n_ctx - 1)
            def _():
                for c in halo:
                    c.wait_send()

            def drain(a, carry):
                @pl.when(a + 2 < n_arr)
                def _():
                    fwd_ring(a).wait_send()
                fwd_part(a).wait_send()
                return carry
            lax.fori_loop(0, n_arr, drain, 0)

            def arrive(a, carry):
                d = theirs(a)
                remote(block(a % 2, d), block(a % 2, d), ps.at[a], pr.at[a], partner).wait_recv()
                return carry
            lax.fori_loop(0, n_arr + 2, arrive, 0)

    flops = 0
    for s, l in stages:
        flops += 2 * rows * width * {"mlp": 3 * ff, "qkv": qw + 2 * kw, "oproj": qw, "lattn": 4 * rows}[s]
    return pl.pallas_call(
        kernel, out_shape=tuple(outs), in_specs=specs, out_specs=tuple(out_specs),
        scratch_shapes=list(scratch.values()),
        cost_estimate=pl.CostEstimate(flops=flops, bytes_accessed=len(mlps) * 3 * width * ff * 2 + 10**6, transcendentals=0),
        compiler_params=pltpu.CompilerParams(vmem_limit_bytes=60 * 1024 * 1024, collective_id=cid, has_side_effects=cid is not None), name=name)(*ins)


CB = 1024


def flash_units(q_ref, m_ref, l_ref, acc_ref, s_scr, k_of, v_of, keys, mask, heads, dim, scale):
    def scores(h):
        return dot_t(q_ref[:, h * dim:(h + 1) * dim], k_of())
    s_scr[0, :, 0:keys] = scores(0)
    for h in range(heads):
        if h + 1 < heads:
            s_scr[(h + 1) % 2, :, 0:keys] = scores(h + 1)
        s = s_scr[h % 2, :, 0:keys]
        if mask is not None:
            s = jnp.where(mask, s, -jnp.inf)
        m_prev = m_ref[h]
        mx = s[:, 0:128]
        for c in range(1, keys // 128):
            mx = jnp.maximum(mx, s[:, c * 128:(c + 1) * 128])
        m_cur = jnp.maximum(m_prev, jnp.max(mx, axis=1, keepdims=True))
        alpha = jnp.exp2((m_prev - m_cur) * scale)
        lsum = alpha * l_ref[h]
        parts = []
        for c in range(keys // 128):
            e = jnp.exp2((s[:, c * 128:(c + 1) * 128] - m_cur) * scale)
            lsum = lsum + e
            parts.append(e.astype(jnp.bfloat16))
        l_ref[h] = lsum
        m_ref[h] = m_cur
        pv = dotf(jnp.concatenate(parts, axis=1), v_of())
        for c in range(dim // 128):
            lo = h * dim + c * 128
            acc_ref[:, lo:lo + 128] = acc_ref[:, lo:lo + 128] * alpha + pv[:, c * 128:(c + 1) * 128]


def global_call(q, k, v, cc, clen, n_ctx, heads=4):
    rows, qw = q.shape
    dim = k.shape[1]
    slots = cc.shape[1]
    ncb = slots // CB
    n_chip = n_ctx // 2
    scale = dim ** -0.5 * LOG2E
    n_arr = 2 * (n_chip - 1)

    def kernel(clen_ref, q_ref, k_ref, v_ref, cc_h, o_ref, kv, m_ref, l_ref, acc_ref, s_scr, cb, csem, rs, rr, ps, pr):
        me = lax.axis_index("ctx")
        z, p = me // 2, me % 2
        way = 1 - 2 * p
        partner = z * 2 + (1 - p)
        succ = ((z + way + n_chip) % n_chip) * 2 + p
        pred = ((z - way + n_chip) % n_chip) * 2 + p

        def mine(s):
            return ((z - way * s + n_chip) % n_chip) * 2 + p

        def theirs(s):
            return ((z + way * s + n_chip) % n_chip) * 2 + (1 - p)

        barrier = pltpu.get_barrier_semaphore()
        for who in (pred, partner):
            pl.semaphore_signal(barrier, inc=1, device_id={"ctx": who}, device_id_type=MESH)
        pl.semaphore_wait(barrier, 2)

        own = (k_ref, v_ref)

        def own_send(t, who, ss, rsem, i):
            return pltpu.make_async_remote_copy(src_ref=own[t], dst_ref=kv.at[t, me], send_sem=ss.at[i], recv_sem=rsem.at[i], device_id={"ctx": who}, device_id_type=MESH)

        def fwd(a, who, ss, rsem, i):
            d = mine(a // 2 + 1)
            return pltpu.make_async_remote_copy(src_ref=kv.at[a % 2, d], dst_ref=kv.at[a % 2, d], send_sem=ss.at[i], recv_sem=rsem.at[i], device_id={"ctx": who}, device_id_type=MESH)

        for t in range(2):
            own_send(t, succ, rs, rr, t).start()
        for t in range(2):
            own_send(t, partner, ps, pr, t).start()

        def wait_arrival(a):
            d = mine(a // 2 + 1)
            pltpu.make_async_remote_copy(src_ref=kv.at[a % 2, d], dst_ref=kv.at[a % 2, d], send_sem=rs.at[a], recv_sem=rr.at[a], device_id={"ctx": pred}, device_id_type=MESH).wait_recv()

        def wait_partner(t, s):
            d = theirs(s)
            pltpu.make_async_remote_copy(src_ref=kv.at[t, d], dst_ref=kv.at[t, d], send_sem=ps.at[2 * s + t], recv_sem=pr.at[2 * s + t], device_id={"ctx": partner}, device_id_type=MESH).wait_recv()

        def handle(a):
            wait_arrival(a)

            @pl.when(a + 2 < n_arr)
            def _():
                fwd(a, succ, rs, rr, a + 2).start()
            fwd(a, partner, ps, pr, a + 2).start()

        def ccopy(i):
            off = pl.multiple_of(i * CB, CB)
            return [pltpu.make_async_copy(cc_h.at[t, pl.ds(off, CB), :], cb.at[t, i % 2], csem.at[t, i % 2]) for t in range(2)]

        for c in ccopy(0):
            c.start()
        m_ref[...] = jnp.full_like(m_ref, -jnp.inf)
        l_ref[...] = jnp.zeros_like(l_ref)
        acc_ref[...] = jnp.zeros_like(acc_ref)
        units = functools.partial(flash_units, q_ref, m_ref, l_ref, acc_ref, s_scr, heads=heads, dim=dim, scale=scale)
        ri = lax.broadcasted_iota(jnp.int32, (rows, rows), 0)
        ci = lax.broadcasted_iota(jnp.int32, (rows, rows), 1)
        units(lambda: k_ref[...], lambda: v_ref[...], rows, ci <= ri)

        def cache_step(masked):
            def body(i, carry):
                for c in ccopy(i):
                    c.wait()

                @pl.when(i + 1 < ncb)
                def _():
                    for c in ccopy(i + 1):
                        c.start()

                @pl.when(i >= 1)
                def _():
                    handle(i - 1)
                mask = None
                if masked:
                    mask = (lax.broadcasted_iota(jnp.int32, (1, CB), 1) + i * CB) < clen_ref[0]
                units(lambda: cb[0, i % 2], lambda: cb[1, i % 2], CB, mask)
                return carry
            return body
        lax.fori_loop(0, ncb // 2, cache_step(False), 0)
        lax.fori_loop(ncb // 2, ncb, cache_step(True), 0)

        def shard(d):
            @pl.when(d < me)
            def _():
                units(lambda: kv[0, d], lambda: kv[1, d], rows, None)

        def new_step(j, carry):
            s = (j + 1) // 2
            odd = j % 2
            d = ((z + way * (1 - 2 * odd) * s + n_chip) % n_chip) * 2 + (p + 1 - odd) % 2

            @pl.when(odd == 1)
            def _():
                @pl.when(s + ncb - 2 < n_arr)
                def _():
                    handle(s + ncb - 2)

            @pl.when(odd == 0)
            def _():
                wait_partner(0, s)
                wait_partner(1, s)

            @pl.when(d < me)
            def _():
                units(lambda: kv[0, d], lambda: kv[1, d], rows, None)
            return carry
        lax.fori_loop(0, n_ctx - 1, new_step, 0)

        for t in range(2):
            own_send(t, succ, rs, rr, t).wait_send()
            own_send(t, partner, ps, pr, t).wait_send()

        def drain(a, carry):
            @pl.when(a + 2 < n_arr)
            def _():
                fwd(a, succ, rs, rr, a + 2).wait_send()
            fwd(a, partner, ps, pr, a + 2).wait_send()
            return carry
        lax.fori_loop(0, n_arr, drain, 0)
        for h in range(heads):
            den = jnp.sum(l_ref[h], axis=1, keepdims=True)
            o_ref[:, h * dim:(h + 1) * dim] = (acc_ref[:, h * dim:(h + 1) * dim] / den).astype(jnp.bfloat16)

    vm = pl.BlockSpec(memory_space=pltpu.VMEM)
    hb = pl.BlockSpec(memory_space=pl.ANY)
    sem = pltpu.SemaphoreType.DMA
    return pl.pallas_call(
        kernel, out_shape=jax.ShapeDtypeStruct((rows, qw), jnp.bfloat16),
        in_specs=[pl.BlockSpec(memory_space=pltpu.SMEM), vm, vm, vm, hb], out_specs=vm,
        scratch_shapes=[
            pltpu.VMEM((2, n_ctx, rows, dim), jnp.bfloat16),
            pltpu.VMEM((heads, rows, 128), jnp.float32), pltpu.VMEM((heads, rows, 128), jnp.float32),
            pltpu.VMEM((rows, qw), jnp.float32), pltpu.VMEM((2, rows, CB), jnp.float32),
            pltpu.VMEM((2, 2, CB, dim), jnp.bfloat16), sem((2, 2)),
            sem((n_arr,)), sem((n_arr,)), sem((n_arr + 2,)), sem((n_arr + 2,))],
        cost_estimate=pl.CostEstimate(flops=4 * rows * qw * (slots + n_ctx * rows), bytes_accessed=4 * slots * dim, transcendentals=0),
        compiler_params=pltpu.CompilerParams(vmem_limit_bytes=60 * 1024 * 1024, collective_id=1, has_side_effects=True), name="gattn")(clen, q, k, v, cc)


def solution(mesh):
    n_ctx = mesh.shape['ctx']
    row_spec = P(('dp', 'ctx'), None)
    cache_spec = P(None, ('dp', 'ctx'), None, None)
    local_spec = P(None, 'dp', None, None)
    in_specs = (row_spec, P('dp'), cache_spec, cache_spec, local_spec, local_spec) + (P(),) * 9

    def device_step(x, cache_len, k_cache, v_cache, k_local, v_local, g_attn, g_mlp, w_q, w_k, w_v, w_o, w_gate, w_up, w_down):
        weights = (g_attn, g_mlp, w_q, w_k, w_v, w_o, w_gate, w_up, w_down)
        n_pairs = k_cache.shape[0]
        flat = lambda a: a.reshape(a.shape[0], a.shape[1], a.shape[2] * a.shape[3])
        local = (flat(k_local), flat(v_local))
        caches = (flat(k_cache), flat(v_cache))
        o = None
        for i in range(n_pairs):
            l = 2 * i
            head = [] if i == 0 else [("oproj", l - 1), ("mlp", l - 1)]
            stages = head + [("qkv", l), ("lattn", l), ("oproj", l), ("mlp", l), ("qkv", l + 1)]
            x, q, k, v, cc = dense_call(stages, x, weights, local=local, caches=caches, pair=i, attn=o, n_ctx=n_ctx, cid=2 + i, name="dense%d" % i)
            o = global_call(q, k, v, cc, cache_len, n_ctx)
        l = 2 * n_pairs - 1
        return dense_call([("oproj", l), ("mlp", l)], x, weights, attn=o, name="last")[0]

    return jax.shard_map(device_step, mesh=mesh, in_specs=in_specs, out_specs=row_spec, check_vma=False)
```

```python
import functools
import jax
import jax.numpy as jnp
from jax import lax
from jax.sharding import PartitionSpec as P
from jax.experimental import pallas as pl
from jax.experimental.pallas import tpu as pltpu

NORM_EPS = 1e-6
LOG2E = 1.4426950408889634
MESH = pl.DeviceIdType.MESH
BF = 768
NS = 2


def rms_rows(x, gain):
    xf = x.astype(jnp.float32)
    inv = lax.rsqrt(jnp.mean(xf * xf, axis=-1, keepdims=True) + NORM_EPS)
    return (xf * inv * gain.astype(jnp.float32)).astype(jnp.bfloat16)


def dotf(a, b):
    return jnp.dot(a, b, preferred_element_type=jnp.float32)


def dot_t(a, b):
    return lax.dot_general(a, b, (((1,), (1,)), ((), ())), preferred_element_type=jnp.float32)


def dense_call(stages, x, weights, local=None, caches=None, pair=0, attn=None, heads=4, n_ctx=0, cid=None, name="dense"):
    g_attn, g_mlp, w_q, w_k, w_v, w_o, w_gate, w_up, w_down = weights
    rows, width = x.shape
    ff = w_gate.shape[-1]
    qw = w_q.shape[-1]
    kw = w_k.shape[-1]
    nb = ff // BF
    names = [s for s, _ in stages]
    has_l = "lattn" in names
    mlps = [l for s, l in stages if s == "mlp"]
    qkvs = [l for s, l in stages if s == "qkv"]
    last_qkv = stages[-1][0] == "qkv"
    n_chip = n_ctx // 2
    n_arr = 2 * (n_chip - 1)
    oprojs = [l for s, l in stages if s == "oproj"]
    scale = kw ** -0.5 * LOG2E

    ins = [x, g_attn, g_mlp]
    vm = pl.BlockSpec(memory_space=pltpu.VMEM)
    hb = pl.BlockSpec(memory_space=pl.ANY)
    specs = [vm] * 3
    if attn is not None:
        ins += [attn]
        specs += [vm]
    n_small = len(ins)
    ins += [w_q, w_k, w_v, w_o, w_gate, w_up, w_down]
    specs += [hb] * 7
    if has_l:
        ins += list(local) + list(caches)
        specs += [hb] * 4
    n_in = len(ins)
    outs = [jax.ShapeDtypeStruct((rows, width), jnp.bfloat16)]
    out_specs = [vm]
    if last_qkv:
        out_specs += [vm] * 3
        outs += [jax.ShapeDtypeStruct((rows, qw), jnp.bfloat16), jax.ShapeDtypeStruct((rows, kw), jnp.bfloat16), jax.ShapeDtypeStruct((rows, kw), jnp.bfloat16)]
    scratch = dict(
        xs=pltpu.VMEM((rows, width), jnp.bfloat16),
        hs=pltpu.VMEM((rows, width), jnp.bfloat16),
        acc=pltpu.VMEM((rows, width), jnp.float32),
        os=pltpu.VMEM((rows, qw), jnp.bfloat16),
        wqb=pltpu.VMEM((width, qw), jnp.bfloat16),
        wkb=pltpu.VMEM((width, kw), jnp.bfloat16),
        wvb=pltpu.VMEM((width, kw), jnp.bfloat16),
        wob=pltpu.VMEM((qw, width), jnp.bfloat16),
        wgb=pltpu.VMEM((NS, width, BF), jnp.bfloat16),
        wub=pltpu.VMEM((NS, width, BF), jnp.bfloat16),
        wdb=pltpu.VMEM((NS, BF, width), jnp.bfloat16),
        msem=pltpu.SemaphoreType.DMA((3, NS)),
        psem=pltpu.SemaphoreType.DMA((4,)),
    )
    if has_l:
        outs += [jax.ShapeDtypeStruct((2, n_ctx * rows, kw), jnp.bfloat16)]
        out_specs += [hb]
        scratch.update(
            kvx=pltpu.VMEM((2, 2 * rows, kw), jnp.bfloat16),
            qs=pltpu.VMEM((rows, qw), jnp.bfloat16),
            own=pltpu.VMEM((2, rows, kw), jnp.bfloat16),
            hsem=pltpu.SemaphoreType.DMA((2, 2)),
            osem=pltpu.SemaphoreType.DMA((2, 2)),
            rs=pltpu.SemaphoreType.DMA((n_arr,)), rr=pltpu.SemaphoreType.DMA((n_arr,)),
            ps=pltpu.SemaphoreType.DMA((n_arr + 2,)), pr=pltpu.SemaphoreType.DMA((n_arr + 2,)),
        )
    keys = list(scratch)

    def kernel(*refs):
        x_ref, ga_ref, gm_ref = refs[:3]
        if attn is not None:
            a_ref = refs[3]
        wq_h, wk_h, wv_h, wo_h, wg_h, wu_h, wd_h = refs[n_small:n_small + 7]
        o_refs = refs[n_in:n_in + len(outs)]
        sc = dict(zip(keys, refs[n_in + len(outs):]))
        xs, hs, acc, os_ = sc["xs"], sc["hs"], sc["acc"], sc["os"]
        sent = [0]

        def wcopies(l, j, slot):
            off = pl.multiple_of(j * BF, BF)
            return [
                pltpu.make_async_copy(wg_h.at[l, :, pl.ds(off, BF)], sc["wgb"].at[slot], sc["msem"].at[0, slot]),
                pltpu.make_async_copy(wu_h.at[l, :, pl.ds(off, BF)], sc["wub"].at[slot], sc["msem"].at[1, slot]),
                pltpu.make_async_copy(wd_h.at[l, pl.ds(off, BF), :], sc["wdb"].at[slot], sc["msem"].at[2, slot]),
            ]

        def start_mlp(l):
            for j in range(NS - 1):
                for c in wcopies(l, j, j):
                    c.start()

        def qkv_copies(l):
            return [pltpu.make_async_copy(src.at[l], sc[dst], sc["psem"].at[i]) for i, (src, dst) in enumerate([(wq_h, "wqb"), (wk_h, "wkb"), (wv_h, "wvb")])]

        def o_copy(l):
            return pltpu.make_async_copy(wo_h.at[l], sc["wob"], sc["psem"].at[3])

        if attn is not None:
            o_copy(oprojs[0]).start()
        if qkvs:
            for c in qkv_copies(qkvs[0]):
                c.start()
        if attn is None:
            o_copy(oprojs[0]).start()
        start_mlp(mlps[0])
        cur = [x_ref]

        if has_l:
            kl_h, vl_h, kc_h, vc_h = refs[n_small + 7:n_in]
            cc = o_refs[-1]
            kvx, qs, own = sc["kvx"], sc["qs"], sc["own"]
            hsem, osem, rs, rr, ps, pr = (sc[n] for n in ("hsem", "osem", "rs", "rr", "ps", "pr"))
            me = lax.axis_index("ctx")
            z, p = me // 2, me % 2
            way = 1 - 2 * p
            partner = z * 2 + (1 - p)
            succ = ((z + way + n_chip) % n_chip) * 2 + p
            pred = ((z - way + n_chip) % n_chip) * 2 + p

            def block(t, d):
                return cc.at[t, pl.ds(pl.multiple_of(d * rows, rows), rows), :]

            def mine(a):
                return ((z - way * (a // 2 + 1) + n_chip) % n_chip) * 2 + p

            def theirs(a):
                return ((z + way * (a // 2) + n_chip) % n_chip) * 2 + (1 - p)

            def remote(src, dst, ssem, rsem, who):
                return pltpu.make_async_remote_copy(src_ref=src, dst_ref=dst, send_sem=ssem, recv_sem=rsem, device_id={"ctx": who}, device_id_type=MESH)

            own_in = [pltpu.make_async_copy(src.at[pair], own.at[t], osem.at[0, t]) for t, src in ((0, kc_h), (1, vc_h))]
            own_out = [pltpu.make_async_copy(own.at[t], block(t, me), osem.at[1, t]) for t in range(2)]
            own_ring = [remote(own.at[t], block(t, me), rs.at[t], rr.at[t], succ) for t in range(2)]
            own_part = [remote(own.at[t], block(t, me), ps.at[t], pr.at[t], partner) for t in range(2)]

            def fwd_ring(a):
                return remote(block(a % 2, mine(a)), block(a % 2, mine(a)), rs.at[a + 2], rr.at[a + 2], succ)

            def fwd_part(a):
                return remote(block(a % 2, mine(a)), block(a % 2, mine(a)), ps.at[a + 2], pr.at[a + 2], partner)

            def handle(a):
                remote(block(a % 2, mine(a)), block(a % 2, mine(a)), rs.at[a], rr.at[a], pred).wait_recv()

                @pl.when(a + 2 < n_arr)
                def _():
                    fwd_ring(a).start()
                fwd_part(a).start()

            halo = [remote(kvx.at[t, pl.ds(rows, rows), :], kvx.at[t, pl.ds(0, rows), :], hsem.at[0, t], hsem.at[1, t], me + 1) for t in range(2)]
            halo_in = [remote(kvx.at[t, pl.ds(rows, rows), :], kvx.at[t, pl.ds(0, rows), :], hsem.at[0, t], hsem.at[1, t], me - 1) for t in range(2)]
            first_in = [pltpu.make_async_copy(src.at[pair], kvx.at[t, pl.ds(0, rows), :], hsem.at[1, t]) for t, src in ((0, kl_h), (1, vl_h))]

            for c in own_in:
                c.start()
            barrier = pltpu.get_barrier_semaphore()
            for who in (pred, partner):
                pl.semaphore_signal(barrier, inc=1, device_id={"ctx": who}, device_id_type=MESH)

            @pl.when(p == 0)
            def _():
                pl.semaphore_signal(barrier, inc=1, device_id={"ctx": (me - 1 + n_ctx) % n_ctx}, device_id_type=MESH)

            @pl.when(me == 0)
            def _():
                for c in first_in:
                    c.start()
            pl.semaphore_wait(barrier, 2 + p)
            for t in range(2):
                own_in[t].wait()
                own_ring[t].start()
                own_part[t].start()
                own_out[t].start()

        def do_lattn(l):
            half = rows // 2

            @pl.when(me == 0)
            def _():
                for c in first_in:
                    c.wait()

            @pl.when(me > 0)
            def _():
                for c in halo_in:
                    c.wait_recv()
            if sent[0] == 1:
                handle(1)
                sent[0] = 2
            span = rows + half
            ri = lax.broadcasted_iota(jnp.int32, (half, span), 0)
            ci = lax.broadcasted_iota(jnp.int32, (half, span), 1)
            ok = (ci > ri) & (ci <= ri + rows)
            for t in range(2):
                for h in range(heads):
                    qt = qs[t * half:(t + 1) * half, h * kw:(h + 1) * kw]
                    s = dot_t(qt, kvx[0, t * half:t * half + span, :])
                    s = jnp.where(ok, s, -jnp.inf)
                    m = jnp.max(s, axis=1, keepdims=True)
                    e = jnp.exp2((s - m) * scale)
                    den = jnp.sum(e, axis=1, keepdims=True)
                    num = dotf(e.astype(jnp.bfloat16), kvx[1, t * half:t * half + span, :])
                    os_[t * half:(t + 1) * half, h * kw:(h + 1) * kw] = (num / den).astype(jnp.bfloat16)

        def do_oproj(l):
            src = a_ref if attn is not None and l == oprojs[0] else os_
            o_copy(l).wait()
            xs[...] = (cur[0][...].astype(jnp.float32) + dotf(src[...], sc["wob"][...])).astype(jnp.bfloat16)
            cur[0] = xs
            if l != oprojs[-1]:
                o_copy(oprojs[-1]).start()

        def do_mlp(l):
            hs[...] = rms_rows(cur[0][...], gm_ref[l:l + 1, :])
            acc[...] = cur[0][...].astype(jnp.float32)

            def step(j, slot, nxt_slot):
                for c in wcopies(l, j, slot):
                    c.wait()

                @pl.when(j + NS - 1 < nb)
                def _():
                    for c in wcopies(l, j + NS - 1, nxt_slot):
                        c.start()
                ga = dotf(hs[...], sc["wgb"][slot])
                up = dotf(hs[...], sc["wub"][slot])
                a = (jax.nn.gelu(ga, approximate=True) * up).astype(jnp.bfloat16)
                acc[...] += dotf(a, sc["wdb"][slot])

            base = sent[0]

            def loop(j, _):
                step(j, lax.rem(j, NS), lax.rem(j + NS - 1, NS))
                if has_l:
                    @pl.when(j + base < n_arr)
                    def _():
                        handle(j + base)
                return 0
            lax.fori_loop(0, nb, loop, 0)
            sent[0] = min(base + nb, n_arr)
            if has_l and l == mlps[-1]:
                for a in range(sent[0], n_arr - 1):
                    handle(a)
                sent[0] = max(sent[0], n_arr - 1)
            if l != mlps[-1]:
                start_mlp(mlps[-1])
            xs[...] = acc[...].astype(jnp.bfloat16)
            cur[0] = xs

        def do_qkv(l):
            hs[...] = rms_rows(cur[0][...], ga_ref[l:l + 1, :])
            for c in qkv_copies(l):
                c.wait()
            to_local = has_l and l == qkvs[0]
            if to_local:
                kvx[0, rows:2 * rows, :] = dotf(hs[...], sc["wkb"][...]).astype(jnp.bfloat16)
                kvx[1, rows:2 * rows, :] = dotf(hs[...], sc["wvb"][...]).astype(jnp.bfloat16)

                @pl.when(me < n_ctx - 1)
                def _():
                    halo[0].start()
                half_q = qw // 2
                qs[:, 0:half_q] = dotf(hs[...], sc["wqb"][:, 0:half_q]).astype(jnp.bfloat16)

                @pl.when(me < n_ctx - 1)
                def _():
                    halo[1].start()
                qs[:, half_q:qw] = dotf(hs[...], sc["wqb"][:, half_q:qw]).astype(jnp.bfloat16)
                for c in qkv_copies(qkvs[1]):
                    c.start()
            else:
                o_refs[2][...] = dotf(hs[...], sc["wkb"][...]).astype(jnp.bfloat16)
                o_refs[3][...] = dotf(hs[...], sc["wvb"][...]).astype(jnp.bfloat16)
                o_refs[1][...] = dotf(hs[...], sc["wqb"][...]).astype(jnp.bfloat16)

        early = 3 if attn is None else 0
        for s, l in stages:
            dict(lattn=do_lattn, oproj=do_oproj, mlp=do_mlp, qkv=do_qkv)[s](l)
            if sent[0] < early and s in ("qkv", "oproj"):
                handle(sent[0])
                sent[0] += 1
        o_refs[0][...] = cur[0][...]
        if has_l:
            for a in range(sent[0], n_arr):
                handle(a)
            for t in range(2):
                own_ring[t].wait_send()
                own_part[t].wait_send()
                own_out[t].wait()

            @pl.when(me < n_ctx - 1)
            def _():
                for c in halo:
                    c.wait_send()

            def drain(a, carry):
                @pl.when(a + 2 < n_arr)
                def _():
                    fwd_ring(a).wait_send()
                fwd_part(a).wait_send()
                return carry
            lax.fori_loop(0, n_arr, drain, 0)

            def arrive(a, carry):
                d = theirs(a)
                remote(block(a % 2, d), block(a % 2, d), ps.at[a], pr.at[a], partner).wait_recv()
                return carry
            lax.fori_loop(0, n_arr + 2, arrive, 0)

    flops = 0
    for s, l in stages:
        flops += 2 * rows * width * {"mlp": 3 * ff, "qkv": qw + 2 * kw, "oproj": qw, "lattn": 4 * rows}[s]
    return pl.pallas_call(
        kernel, out_shape=tuple(outs), in_specs=specs, out_specs=tuple(out_specs),
        scratch_shapes=list(scratch.values()),
        cost_estimate=pl.CostEstimate(flops=flops, bytes_accessed=len(mlps) * 3 * width * ff * 2 + 10**6, transcendentals=0),
        compiler_params=pltpu.CompilerParams(vmem_limit_bytes=60 * 1024 * 1024, collective_id=cid, has_side_effects=cid is not None), name=name)(*ins)


CB = 1024


def flash_units(q_ref, m_ref, l_ref, acc_ref, s_scr, k_of, v_of, keys, mask, heads, dim, scale):
    def scores(h):
        return dot_t(q_ref[:, h * dim:(h + 1) * dim], k_of())
    s_scr[0, :, 0:keys] = scores(0)
    for h in range(heads):
        if h + 1 < heads:
            s_scr[(h + 1) % 2, :, 0:keys] = scores(h + 1)
        s = s_scr[h % 2, :, 0:keys]
        if mask is not None:
            s = jnp.where(mask, s, -jnp.inf)
        m_prev = m_ref[h]
        mx = s[:, 0:128]
        for c in range(1, keys // 128):
            mx = jnp.maximum(mx, s[:, c * 128:(c + 1) * 128])
        m_cur = jnp.maximum(m_prev, jnp.max(mx, axis=1, keepdims=True))
        alpha = jnp.exp2((m_prev - m_cur) * scale)
        lsum = alpha * l_ref[h]
        parts = []
        for c in range(keys // 128):
            e = jnp.exp2((s[:, c * 128:(c + 1) * 128] - m_cur) * scale)
            lsum = lsum + e
            parts.append(e.astype(jnp.bfloat16))
        l_ref[h] = lsum
        m_ref[h] = m_cur
        pv = dotf(jnp.concatenate(parts, axis=1), v_of())
        for c in range(dim // 128):
            lo = h * dim + c * 128
            acc_ref[:, lo:lo + 128] = acc_ref[:, lo:lo + 128] * alpha + pv[:, c * 128:(c + 1) * 128]


def global_call(q, k, v, cc, clen, n_ctx, heads=4):
    rows, qw = q.shape
    dim = k.shape[1]
    slots = cc.shape[1]
    ncb = slots // CB
    n_chip = n_ctx // 2
    scale = dim ** -0.5 * LOG2E
    n_arr = 2 * (n_chip - 1)

    def kernel(clen_ref, q_ref, k_ref, v_ref, cc_h, o_ref, kv, m_ref, l_ref, acc_ref, s_scr, cb, csem, rs, rr, ps, pr):
        me = lax.axis_index("ctx")
        z, p = me // 2, me % 2
        way = 1 - 2 * p
        partner = z * 2 + (1 - p)
        succ = ((z + way + n_chip) % n_chip) * 2 + p
        pred = ((z - way + n_chip) % n_chip) * 2 + p

        def mine(s):
            return ((z - way * s + n_chip) % n_chip) * 2 + p

        def theirs(s):
            return ((z + way * s + n_chip) % n_chip) * 2 + (1 - p)

        barrier = pltpu.get_barrier_semaphore()
        for who in (pred, partner):
            pl.semaphore_signal(barrier, inc=1, device_id={"ctx": who}, device_id_type=MESH)
        pl.semaphore_wait(barrier, 2)

        own = (k_ref, v_ref)

        def own_send(t, who, ss, rsem, i):
            return pltpu.make_async_remote_copy(src_ref=own[t], dst_ref=kv.at[t, me], send_sem=ss.at[i], recv_sem=rsem.at[i], device_id={"ctx": who}, device_id_type=MESH)

        def fwd(a, who, ss, rsem, i):
            d = mine(a // 2 + 1)
            return pltpu.make_async_remote_copy(src_ref=kv.at[a % 2, d], dst_ref=kv.at[a % 2, d], send_sem=ss.at[i], recv_sem=rsem.at[i], device_id={"ctx": who}, device_id_type=MESH)

        for t in range(2):
            own_send(t, succ, rs, rr, t).start()
        for t in range(2):
            own_send(t, partner, ps, pr, t).start()

        def wait_arrival(a):
            d = mine(a // 2 + 1)
            pltpu.make_async_remote_copy(src_ref=kv.at[a % 2, d], dst_ref=kv.at[a % 2, d], send_sem=rs.at[a], recv_sem=rr.at[a], device_id={"ctx": pred}, device_id_type=MESH).wait_recv()

        def wait_partner(t, s):
            d = theirs(s)
            pltpu.make_async_remote_copy(src_ref=kv.at[t, d], dst_ref=kv.at[t, d], send_sem=ps.at[2 * s + t], recv_sem=pr.at[2 * s + t], device_id={"ctx": partner}, device_id_type=MESH).wait_recv()

        def handle(a):
            wait_arrival(a)

            @pl.when(a + 2 < n_arr)
            def _():
                fwd(a, succ, rs, rr, a + 2).start()
            fwd(a, partner, ps, pr, a + 2).start()

        def ccopy(i):
            off = pl.multiple_of(i * CB, CB)
            return [pltpu.make_async_copy(cc_h.at[t, pl.ds(off, CB), :], cb.at[t, i % 2], csem.at[t, i % 2]) for t in range(2)]

        for c in ccopy(0):
            c.start()
        m_ref[...] = jnp.full_like(m_ref, -jnp.inf)
        l_ref[...] = jnp.zeros_like(l_ref)
        acc_ref[...] = jnp.zeros_like(acc_ref)
        units = functools.partial(flash_units, q_ref, m_ref, l_ref, acc_ref, s_scr, heads=heads, dim=dim, scale=scale)
        ri = lax.broadcasted_iota(jnp.int32, (rows, rows), 0)
        ci = lax.broadcasted_iota(jnp.int32, (rows, rows), 1)
        units(lambda: k_ref[...], lambda: v_ref[...], rows, ci <= ri)

        def cache_step(masked):
            def body(i, carry):
                for c in ccopy(i):
                    c.wait()

                @pl.when(i + 1 < ncb)
                def _():
                    for c in ccopy(i + 1):
                        c.start()

                @pl.when(i >= 1)
                def _():
                    handle(i - 1)
                mask = None
                if masked:
                    mask = (lax.broadcasted_iota(jnp.int32, (1, CB), 1) + i * CB) < clen_ref[0]
                units(lambda: cb[0, i % 2], lambda: cb[1, i % 2], CB, mask)
                return carry
            return body
        lax.fori_loop(0, ncb // 2, cache_step(False), 0)
        lax.fori_loop(ncb // 2, ncb, cache_step(True), 0)

        def shard(d):
            @pl.when(d < me)
            def _():
                units(lambda: kv[0, d], lambda: kv[1, d], rows, None)

        def new_step(j, carry):
            s = (j + 1) // 2
            odd = j % 2
            d = ((z + way * (1 - 2 * odd) * s + n_chip) % n_chip) * 2 + (p + 1 - odd) % 2

            @pl.when(odd == 1)
            def _():
                @pl.when(s + ncb - 2 < n_arr)
                def _():
                    handle(s + ncb - 2)

            @pl.when(odd == 0)
            def _():
                wait_partner(0, s)
                wait_partner(1, s)

            @pl.when(d < me)
            def _():
                units(lambda: kv[0, d], lambda: kv[1, d], rows, None)
            return carry
        lax.fori_loop(0, n_ctx - 1, new_step, 0)

        for t in range(2):
            own_send(t, succ, rs, rr, t).wait_send()
            own_send(t, partner, ps, pr, t).wait_send()

        def drain(a, carry):
            @pl.when(a + 2 < n_arr)
            def _():
                fwd(a, succ, rs, rr, a + 2).wait_send()
            fwd(a, partner, ps, pr, a + 2).wait_send()
            return carry
        lax.fori_loop(0, n_arr, drain, 0)
        for h in range(heads):
            den = jnp.sum(l_ref[h], axis=1, keepdims=True)
            o_ref[:, h * dim:(h + 1) * dim] = (acc_ref[:, h * dim:(h + 1) * dim] / den).astype(jnp.bfloat16)

    vm = pl.BlockSpec(memory_space=pltpu.VMEM)
    hb = pl.BlockSpec(memory_space=pl.ANY)
    sem = pltpu.SemaphoreType.DMA
    return pl.pallas_call(
        kernel, out_shape=jax.ShapeDtypeStruct((rows, qw), jnp.bfloat16),
        in_specs=[pl.BlockSpec(memory_space=pltpu.SMEM), vm, vm, vm, hb], out_specs=vm,
        scratch_shapes=[
            pltpu.VMEM((2, n_ctx, rows, dim), jnp.bfloat16),
            pltpu.VMEM((heads, rows, 128), jnp.float32), pltpu.VMEM((heads, rows, 128), jnp.float32),
            pltpu.VMEM((rows, qw), jnp.float32), pltpu.VMEM((2, rows, CB), jnp.float32),
            pltpu.VMEM((2, 2, CB, dim), jnp.bfloat16), sem((2, 2)),
            sem((n_arr,)), sem((n_arr,)), sem((n_arr + 2,)), sem((n_arr + 2,))],
        cost_estimate=pl.CostEstimate(flops=4 * rows * qw * (slots + n_ctx * rows), bytes_accessed=4 * slots * dim, transcendentals=0),
        compiler_params=pltpu.CompilerParams(vmem_limit_bytes=60 * 1024 * 1024, collective_id=1, has_side_effects=True), name="gattn")(clen, q, k, v, cc)


def solution(mesh):
    n_ctx = mesh.shape['ctx']
    row_spec = P(('dp', 'ctx'), None)
    cache_spec = P(None, ('dp', 'ctx'), None, None)
    local_spec = P(None, 'dp', None, None)
    in_specs = (row_spec, P('dp'), cache_spec, cache_spec, local_spec, local_spec) + (P(),) * 9

    def device_step(x, cache_len, k_cache, v_cache, k_local, v_local, g_attn, g_mlp, w_q, w_k, w_v, w_o, w_gate, w_up, w_down):
        weights = (g_attn, g_mlp, w_q, w_k, w_v, w_o, w_gate, w_up, w_down)
        n_pairs = k_cache.shape[0]
        flat = lambda a: a.reshape(a.shape[0], a.shape[1], a.shape[2] * a.shape[3])
        local = (flat(k_local), flat(v_local))
        caches = (flat(k_cache), flat(v_cache))
        o = None
        for i in range(n_pairs):
            l = 2 * i
            head = [] if i == 0 else [("oproj", l - 1), ("mlp", l - 1)]
            stages = head + [("qkv", l), ("lattn", l), ("oproj", l), ("mlp", l), ("qkv", l + 1)]
            x, q, k, v, cc = dense_call(stages, x, weights, local=local, caches=caches, pair=i, attn=o, n_ctx=n_ctx, cid=2 + i, name="dense%d" % i)
            o = global_call(q, k, v, cc, cache_len, n_ctx)
        l = 2 * n_pairs - 1
        return dense_call([("oproj", l), ("mlp", l)], x, weights, attn=o, name="last")[0]

    return jax.shard_map(device_step, mesh=mesh, in_specs=in_specs, out_specs=row_spec, check_vma=False)
```
